256 devices in a mesh: seg: 16 (over y_hi, x, core), tok: 16 (over z, y_lo).
Axes of the slice: x: 4, y: 4 (y_hi: 2, y_lo: 2; y = y_hi * 2 + y_lo), z: 8, core: 2. Of those that a mesh axis runs over, the one named last changes fastest.
Arguments:
- value: bfloat16 [1048576, 128], P(('seg', 'tok')), may hold values from -6 to 6
- gate_in: bfloat16 [1048576, 128], P(('seg', 'tok')), may hold values from -6 to 6
- gate_out: bfloat16 [1048576, 128], P(('seg', 'tok')), may hold values from -6 to 6
- filter_spectrum: bfloat16 [2, 256, 512, 128], P(None, 'tok'), may hold values from -8 to 8, as said below
- skip_gain: float32 [128], replicated, may hold values from 0.25 to 2
Outputs:
- mixed_out: bfloat16 [1048576, 128], P(('seg', 'tok'))
The draws below stay inside these ranges and needn't reach their ends.
Inputs may be any that keep to these rules, and one draw needn't show every extreme that they name: `filter_spectrum`: the response of a real filter whose taps beyond the first 65536 are zero, rounded.
All inputs are finite; a program needn't handle non-finite values.
Results may differ from the reference program's by a relative error of at most 0.0085.
Values may be sent and summed in bfloat16 or wider, within the bound.
No kernel may reach another device: no remote copies, remote signals or barrier semaphores. Data moves between devices by JAX's collectives and lax.ppermute only.
A program may use at most 128 MiB of HBM per device.

```python
import math
import jax
import jax.numpy as jnp
from jax import lax

SEG = 65536
N1 = 256
N2 = 512
CH = 128
TOKENS = 1048576
N_SEG = 16


def angle_tables(row_count, col_count, modulus):
    rows = jnp.arange(row_count, dtype=jnp.int32)
    cols = jnp.arange(col_count, dtype=jnp.int32)
    product = rows[:, None] * cols[None, :] % modulus
    angle = product.astype(jnp.float32) * jnp.float32(2.0 * math.pi / modulus)
    return (jnp.cos(angle), jnp.sin(angle))


def draw_filter_spectrum(key, part):
    taps_key, rate_key = jax.random.split(jax.random.fold_in(key, 7))
    rates = jnp.exp(jax.random.uniform(rate_key, (CH,), jnp.float32, math.log(0.25), math.log(400.0))) / SEG
    position = jnp.arange(SEG, dtype=jnp.float32)
    envelope = jnp.exp(-position[:, None] * rates[None, :]) * jnp.sqrt(1.0 - jnp.exp(-2.0 * rates))[None, :]
    noise = jax.random.normal(taps_key, (SEG, CH), jnp.float32)
    taps = (noise * envelope).reshape(N1 // 2, N2, CH)
    cos_one, sin_one = angle_tables(N1, N1 // 2, N1)
    high = lax.Precision.HIGHEST
    a_real = jnp.einsum('kj,jnc->knc', cos_one, taps, precision=high)
    a_imag = -jnp.einsum('kj,jnc->knc', sin_one, taps, precision=high)
    tw_cos, tw_sin = angle_tables(N1, N2, 2 * SEG)
    tw_cos = tw_cos[:, :, None]
    tw_sin = tw_sin[:, :, None]
    b_real = a_real * tw_cos + a_imag * tw_sin
    b_imag = a_imag * tw_cos - a_real * tw_sin
    cos_two, sin_two = angle_tables(N2, N2, N2)
    x_real = jnp.einsum('knc,nm->kmc', b_real, cos_two, precision=high) + jnp.einsum('knc,nm->kmc', b_imag, sin_two, precision=high)
    x_imag = jnp.einsum('knc,nm->kmc', b_imag, cos_two, precision=high) - jnp.einsum('knc,nm->kmc', b_real, sin_two, precision=high)
    both = jnp.stack([x_real, x_imag])
    return jnp.clip(both, -8.0, 8.0).astype(jnp.bfloat16)


def block_scale(key, extent, cuts, low, high):
    factor_of = 1.0
    for axis_at, parts in cuts:
        steps = jax.random.uniform(jax.random.fold_in(jax.random.fold_in(key, 6), axis_at), (parts,), jnp.float32, low / len(cuts), high / len(cuts))
        factor_of = factor_of * jnp.repeat(jnp.exp(steps), extent[axis_at] // parts).reshape((-1,) + (1,) * (len(extent) - 1 - axis_at))
    return factor_of


def normal_values(stream_key, shape, deviation, limit, cuts=(), kind=jnp.bfloat16):
    values = deviation * jax.random.normal(stream_key, shape, jnp.float32)
    if cuts:
        values = values * block_scale(stream_key, shape, cuts, -0.22, 0.18)
    return jnp.clip(values, -limit, limit).astype(kind)


def setup_inputs(seed: int = 0) -> dict:
    key_list = jax.random.split(jax.random.key(seed), 6)
    value = normal_values(key_list[0], (TOKENS, CH), 1.0, 6.0, ((0, 256),))
    gate_in = normal_values(key_list[1], (TOKENS, CH), 1.0, 6.0, ((0, 256),))
    gate_out = normal_values(key_list[2], (TOKENS, CH), 1.0, 6.0, ((0, 256),))
    filter_spectrum = draw_filter_spectrum(jax.random.fold_in(key_list[5], 71), 0)
    skip_gain = jnp.clip(jnp.exp(jax.random.uniform(key_list[4], (CH,), jnp.float32, math.log(0.25), math.log(2.0))), 0.25, 2.0)
    return dict(value=value, gate_in=gate_in, gate_out=gate_out, filter_spectrum=filter_spectrum, skip_gain=skip_gain)


def span_ids(count):
    return jnp.arange(count, dtype=jnp.int32)


def trig_tables(row_ids, col_ids, modulus):
    product = (row_ids[:, None] * col_ids[None, :]) % modulus
    angle = product.astype(jnp.float32) * jnp.float32(2.0 * math.pi / modulus)
    return jnp.cos(angle), jnp.sin(angle)


def einsum_rows(data, table):
    return jnp.einsum("jnc,nk->jkc", data.astype(jnp.float32), table.astype(jnp.float32))


def reference(value, gate_in, gate_out, filter_spectrum, skip_gain):
    gated = (value.astype(jnp.float32) * gate_in.astype(jnp.float32)).astype(jnp.bfloat16)
    fft_len = N1 * N2
    half_rows = N1 // 2
    cos_one, sin_one = trig_tables(span_ids(N1), span_ids(half_rows), N1)
    cos_one_b = cos_one.astype(jnp.bfloat16)
    nsin_one_b = (-sin_one).astype(jnp.bfloat16)
    cos_two, sin_two = trig_tables(span_ids(N2), span_ids(N2), N2)
    cos_two_b = cos_two.astype(jnp.bfloat16)
    sin_two_b = sin_two.astype(jnp.bfloat16)
    inv_cos, inv_sin = trig_tables(span_ids(N1), span_ids(N1), N1)
    inv_cos_b = inv_cos.astype(jnp.bfloat16)
    inv_nsin_b = (-inv_sin).astype(jnp.bfloat16)
    tw_cos, tw_sin = trig_tables(span_ids(N1), span_ids(N2), fft_len)
    tw_cos = tw_cos[:, :, None]
    tw_sin = tw_sin[:, :, None]
    h_real = filter_spectrum[0].astype(jnp.float32)
    h_imag = filter_spectrum[1].astype(jnp.float32)
    scale = jnp.float32(1.0 / fft_len)

    def one_segment(segment):
        flat = segment.reshape(half_rows, N2 * CH)
        a_real = jnp.dot(cos_one_b, flat, preferred_element_type=jnp.float32).reshape(N1, N2, CH)
        a_imag = jnp.dot(nsin_one_b, flat, preferred_element_type=jnp.float32).reshape(N1, N2, CH)
        b_real = (a_real * tw_cos + a_imag * tw_sin).astype(jnp.bfloat16)
        b_imag = (a_imag * tw_cos - a_real * tw_sin).astype(jnp.bfloat16)
        x_real = einsum_rows(b_real, cos_two_b) + einsum_rows(b_imag, sin_two_b)
        x_imag = einsum_rows(b_imag, cos_two_b) - einsum_rows(b_real, sin_two_b)
        z_real = (x_real * h_real - x_imag * h_imag).astype(jnp.bfloat16)
        z_imag = (x_real * h_imag + x_imag * h_real).astype(jnp.bfloat16)
        p_real = einsum_rows(z_real, cos_two_b) - einsum_rows(z_imag, sin_two_b)
        p_imag = einsum_rows(z_imag, cos_two_b) + einsum_rows(z_real, sin_two_b)
        q_real = (p_real * tw_cos - p_imag * tw_sin).astype(jnp.bfloat16)
        q_imag = (p_imag * tw_cos + p_real * tw_sin).astype(jnp.bfloat16)
        total = jnp.dot(inv_cos_b, q_real.reshape(N1, N2 * CH), preferred_element_type=jnp.float32)
        total = total + jnp.dot(inv_nsin_b, q_imag.reshape(N1, N2 * CH), preferred_element_type=jnp.float32)
        return (total * scale).astype(jnp.bfloat16).reshape(fft_len, CH)

    segments = gated.reshape(N_SEG, half_rows, N2, CH)
    convs = lax.map(one_segment, segments)
    main_part = convs[:, :SEG]
    tail_part = convs[:, SEG:]
    carried = jnp.concatenate([jnp.zeros((1, SEG, CH), jnp.bfloat16), tail_part[:-1]], axis=0)
    mixed = (main_part.astype(jnp.float32) + carried.astype(jnp.float32)).astype(jnp.bfloat16)
    mixed = mixed.reshape(TOKENS, CH)
    result = gate_out.astype(jnp.float32) * (mixed.astype(jnp.float32) + skip_gain[None, :] * gated.astype(jnp.float32))
    return result.astype(jnp.bfloat16)
```

```python
import functools
import math

import jax
import jax.numpy as jnp
import numpy as np
from jax import lax
from jax.experimental import pallas as pl
from jax.experimental.pallas import tpu as pltpu
from jax.sharding import Mesh, PartitionSpec as P

N1 = 256
N2 = 512
HALF = N2 // 2
ROWS = N1 // 2
FFT = N1 * N2
LANES = 128
SEGS = 8
ROW_T = 8
WIDE = N2 + LANES

ALL = ("yh", "x", "core", "z", "yl")
GROUP = ("x", "core", "z", "yl")


def trig(rows, cols, modulus):
    product = (rows[:, None].astype(np.int64) * cols[None, :]) % modulus
    angle = product.astype(np.float64) * (2.0 * math.pi / modulus)
    return np.cos(angle), np.sin(angle)


def tables():
    rh, t, row = np.meshgrid(np.arange(2), np.arange(16), np.arange(8), indexing="ij")
    k1 = (16 * t + 8 * rh + row).reshape(-1)
    n1 = np.arange(N1)
    n2 = np.arange(N2)
    k2 = np.arange(HALF)
    cos_one, sin_one = trig(k1, n1, N1)
    first = np.concatenate([cos_one, -sin_one], axis=0)
    cos_two, sin_two = trig(n2, k2, N2)
    tw_cos, tw_sin = trig(k1, n2, FFT)
    last = np.concatenate([cos_one.T[:ROWS], -sin_one.T[:ROWS]], axis=1)
    half = lambda a: jnp.asarray(a, jnp.float32).astype(jnp.bfloat16)
    return (
        np.asarray(first, dtype=jnp.bfloat16),
        np.asarray(cos_two, dtype=jnp.bfloat16),
        np.asarray(sin_two, dtype=jnp.bfloat16),
        np.asarray(cos_two.T, dtype=jnp.bfloat16),
        np.asarray(sin_two.T, dtype=jnp.bfloat16),
        np.asarray(tw_cos, dtype=np.float32),
        np.asarray(tw_sin, dtype=np.float32),
        np.asarray(last, dtype=jnp.bfloat16),
    )


def conv_body(cur, prev, h_re, h_im, first, c2, s2, c3, s3, tc, ts, last, out):
    dot = functools.partial(jnp.dot, preferred_element_type=jnp.float32)
    data = jnp.concatenate([cur[...], prev[...]], axis=0)
    a = dot(first[...], data)
    a_re = a[:N1]
    a_im = a[N1:]
    tcv = tc[...]
    tsv = ts[...]
    b_re = a_re * tcv + a_im * tsv
    b_im = a_im * tcv - a_re * tsv
    parity = lax.broadcasted_iota(jnp.int32, (1, N2), 1) % 2
    sign = (1 - 2 * parity).astype(jnp.float32)
    nyq = jnp.sum(a_re[0:1] * sign, axis=1, keepdims=True)
    b_re = b_re.astype(jnp.bfloat16)
    b_im = b_im.astype(jnp.bfloat16)
    x_re = dot(b_re, c2[...]) + dot(b_im, s2[...])
    x_im = dot(b_im, c2[...]) - dot(b_re, s2[...])
    hr = h_re.astype(jnp.float32)
    hi = h_im.astype(jnp.float32)
    z_re = (x_re * hr - x_im * hi).astype(jnp.bfloat16)
    z_im = (x_re * hi + x_im * hr).astype(jnp.bfloat16)
    p_re = dot(z_re, c3[...]) - dot(z_im, s3[...])
    p_im = dot(z_im, c3[...]) + dot(z_re, s3[...])
    q_re = (p_re * tcv - p_im * tsv).astype(jnp.bfloat16)
    q_im = (p_im * tcv + p_re * tsv).astype(jnp.bfloat16)
    lastv = last[...]
    total = dot(lastv[:, :N1], q_re) + dot(lastv[:, N1:], q_im)
    total = total + (nyq * hi[0:1, 0:1]) * sign
    out[...] = (total * (2.0 / FFT)).astype(jnp.bfloat16)


def filter_parts(h):
    def part(p):
        rows = []
        for rh in range(2):
            rows.append(jnp.concatenate([h[p * 4 + rh * 2], h[p * 4 + rh * 2 + 1]], axis=1))
        return jnp.concatenate(rows, axis=0)

    return part(0), part(1)


def inner_kernel(cur, prev, h, *rest):
    h_re, h_im = filter_parts(h)
    conv_body(cur.at[0], prev.at[0], h_re, h_im, *rest[:-1], rest[-1].at[0])


def border_kernel(acc, cur, prev, h, *rest):
    h_re, h_im = filter_parts(h)
    conv_body(cur.at[0], prev.at[0], h_re, h_im, *rest[:-1], rest[-1].at[0])


def whole(a):
    return pl.BlockSpec(a.shape, lambda *_: (0,) * a.ndim)


FLOPS = 2 * (2 * N1 * N1 * N2 + 8 * N1 * N2 * HALF + ROWS * 2 * N1 * N2)


def convolve(recv, border, consts):
    hspec = pl.BlockSpec((SEGS, ROWS, LANES), lambda *_: (0, 0, N2 // LANES))
    params = pltpu.CompilerParams(vmem_limit_bytes=50 * 1024 * 1024)
    consts_spec = [whole(c) for c in consts]
    blk = (1, ROWS, N2)
    shape = jax.ShapeDtypeStruct((SEGS, ROWS, N2), jnp.bfloat16)
    inner = pl.pallas_call(
        inner_kernel,
        grid=(SEGS - 1,),
        in_specs=[
            pl.BlockSpec(blk, lambda i: (i + 1, 0, 0)),
            pl.BlockSpec(blk, lambda i: (i, 0, 0)),
            hspec,
        ]
        + consts_spec,
        out_specs=pl.BlockSpec(blk, lambda i: (i + 1, 0, 0)),
        out_shape=shape,
        compiler_params=params,
        cost_estimate=pl.CostEstimate(flops=7 * FLOPS, bytes_accessed=4 << 20, transcendentals=0),
        name="inner",
    )(recv, recv, recv, *consts)
    return pl.pallas_call(
        border_kernel,
        grid=(1,),
        in_specs=[
            pl.BlockSpec(memory_space=pl.ANY),
            pl.BlockSpec(blk, lambda i: (0, 0, 0)),
            pl.BlockSpec(blk, lambda i: (0, 0, 0)),
            hspec,
        ]
        + consts_spec,
        out_specs=pl.BlockSpec(blk, lambda i: (0, 0, 0)),
        out_shape=shape,
        input_output_aliases={0: 0},
        compiler_params=params,
        cost_estimate=pl.CostEstimate(flops=FLOPS, bytes_accessed=3 << 20, transcendentals=0),
        name="border",
    )(inner, recv, border, recv, *consts)


def shards(value, gate_in, gate_out, filter_spectrum, skip_gain):
    sl = lax.axis_index(("x", "core"))
    tok = lax.axis_index(("z", "yl"))
    channels = value.shape[1]
    gated = (value.astype(jnp.float32) * gate_in.astype(jnp.float32)).astype(jnp.bfloat16)
    part = sl // 4
    rh = (sl // 2) % 2
    kh = sl % 2
    piece = lax.dynamic_slice(
        filter_spectrum, (part, rh * ROW_T, kh * LANES, 0), (1, ROW_T, LANES, channels)
    )[0]
    edge = jnp.where(part == 0, piece[0, 0], filter_spectrum[0, 0, HALF])
    edge = edge * jnp.bfloat16(0.5)
    mine = (tok == 0) & (rh == 0) & (kh == 0)
    at_edge = (
        (lax.broadcasted_iota(jnp.int32, piece.shape, 0) == 0)
        & (lax.broadcasted_iota(jnp.int32, piece.shape, 1) == 0)
        & mine
    )
    piece = jnp.where(at_edge, edge[None, None, :], piece)
    send = jnp.concatenate([gated.reshape(ROW_T, N2, channels), piece], axis=1)
    send = jnp.transpose(send, (2, 0, 1))
    recv = lax.all_to_all(send, GROUP, split_axis=0, concat_axis=0, tiled=True)
    recv = recv.reshape(SEGS, ROWS, WIDE)
    border = lax.ppermute(recv[SEGS - 1 :, :, :N2], "yh", [(0, 1)])
    mixed = convolve(recv, border, tables())
    back = lax.all_to_all(
        mixed.reshape(SEGS * 16, ROW_T, N2), GROUP, split_axis=0, concat_axis=0, tiled=True
    )
    mixed = jnp.transpose(back, (1, 2, 0)).reshape(-1, channels)
    result = gate_out.astype(jnp.float32) * (
        mixed.astype(jnp.float32) + skip_gain[None, :] * gated.astype(jnp.float32)
    )
    return result.astype(jnp.bfloat16)


def solution(mesh):
    fine = Mesh(mesh.devices.reshape(2, 4, 2, 8, 2), ALL)
    return jax.shard_map(
        shards,
        mesh=fine,
        in_specs=(
            P(ALL, None),
            P(ALL, None),
            P(ALL, None),
            P(None, ("z", "yl"), None, None),
            P(),
        ),
        out_specs=P(ALL, None),
        check_vma=False,
    )
```

```python
import functools
import math

import jax
import jax.numpy as jnp
import numpy as np
from jax import lax
from jax.experimental import pallas as pl
from jax.experimental.pallas import tpu as pltpu
from jax.sharding import Mesh, PartitionSpec as P

N1 = 256
N2 = 512
HALF = N2 // 2
ROWS = N1 // 2
FFT = N1 * N2
LANES = 128
SEGS = 8
ROW_T = 8
WIDE = N2 + LANES

ALL = ("yh", "x", "core", "z", "yl")
GROUP = ("x", "core", "z", "yl")


def trig(rows, cols, modulus):
    product = (rows[:, None].astype(np.int64) * cols[None, :]) % modulus
    angle = product.astype(np.float64) * (2.0 * math.pi / modulus)
    return np.cos(angle), np.sin(angle)


def tables():
    rh, t, row = np.meshgrid(np.arange(2), np.arange(16), np.arange(8), indexing="ij")
    k1 = (16 * t + 8 * rh + row).reshape(-1)
    n1 = np.arange(N1)
    n2 = np.arange(N2)
    k2 = np.arange(HALF)
    cos_one, sin_one = trig(k1, n1, N1)
    first = np.concatenate([cos_one, -sin_one], axis=0)
    cos_two, sin_two = trig(n2, k2, N2)
    tw_cos, tw_sin = trig(k1, n2, FFT)
    last = np.concatenate([cos_one.T[:ROWS], -sin_one.T[:ROWS]], axis=1)
    half = lambda a: jnp.asarray(a, jnp.float32).astype(jnp.bfloat16)
    return (
        np.asarray(first, dtype=jnp.bfloat16),
        np.asarray(cos_two, dtype=jnp.bfloat16),
        np.asarray(sin_two, dtype=jnp.bfloat16),
        np.asarray(cos_two.T, dtype=jnp.bfloat16),
        np.asarray(sin_two.T, dtype=jnp.bfloat16),
        np.asarray(tw_cos, dtype=np.float32),
        np.asarray(tw_sin, dtype=np.float32),
        np.asarray(last, dtype=jnp.bfloat16),
    )


def dot(a, b):
    return jnp.dot(a, b, preferred_element_type=jnp.float32)


def one_segment(cur, prev, h_re, h_im, first, c2, s2, c3, s3, tc, ts, last):
    data = jnp.concatenate([cur, prev], axis=0)
    a = dot(first[...], data)
    a_re = a[:N1]
    a_im = a[N1:]
    b_re = (a_re * tc[...] + a_im * ts[...]).astype(jnp.bfloat16)
    b_im = (a_im * tc[...] - a_re * ts[...]).astype(jnp.bfloat16)
    parity = lax.broadcasted_iota(jnp.int32, (1, N2), 1) % 2
    sign = (1 - 2 * parity).astype(jnp.float32)
    nyq = jnp.sum(a_re[0:1] * sign, axis=1, keepdims=True)
    x_re = dot(b_re, c2[...]) + dot(b_im, s2[...])
    x_im = dot(b_im, c2[...]) - dot(b_re, s2[...])
    hr = h_re[...]
    hi = h_im[...]
    z_re = (x_re * hr - x_im * hi).astype(jnp.bfloat16)
    z_im = (x_re * hi + x_im * hr).astype(jnp.bfloat16)
    p_re = dot(z_re, c3[...]) - dot(z_im, s3[...])
    p_im = dot(z_im, c3[...]) + dot(z_re, s3[...])
    q_re = (p_re * tc[...] - p_im * ts[...]).astype(jnp.bfloat16)
    q_im = (p_im * tc[...] + p_re * ts[...]).astype(jnp.bfloat16)
    total = dot(last[:, :N1], q_re) + dot(last[:, N1:], q_im)
    total = total + (nyq * h_im[0:1, 0:1]) * sign
    return (total * (2.0 / FFT)).astype(jnp.bfloat16)


def filter_parts(recv, h_re, h_im):
    for p, ref in enumerate((h_re, h_im)):
        for rh in range(2):
            for kh in range(2):
                ref[rh * ROWS : (rh + 1) * ROWS, kh * LANES : (kh + 1) * LANES] = recv[
                    p * 4 + rh * 2 + kh, :, N2:
                ].astype(jnp.float32)


def inner_kernel(recv, first, c2, s2, c3, s3, tc, ts, last, out, h_re, h_im):
    filter_parts(recv, h_re, h_im)

    def step(s, carry):
        out[s] = one_segment(
            recv[s, :, :N2], recv[s - 1, :, :N2], h_re, h_im, first, c2, s2, c3, s3, tc, ts, last
        )
        return carry

    lax.fori_loop(1, SEGS, step, 0)


def border_kernel(acc, recv, border, first, c2, s2, c3, s3, tc, ts, last, out, h_re, h_im):
    filter_parts(recv, h_re, h_im)
    out[0] = one_segment(
        recv[0, :, :N2], border[...], h_re, h_im, first, c2, s2, c3, s3, tc, ts, last
    )


MACS = 2 * N1 * N1 * N2 + 8 * N1 * N2 * HALF + ROWS * 2 * N1 * N2
IN_VMEM = pl.BlockSpec(memory_space=pltpu.VMEM)


def convolve(recv, border, consts):
    params = pltpu.CompilerParams(vmem_limit_bytes=40 * 1024 * 1024)
    shape = jax.ShapeDtypeStruct((SEGS, ROWS, N2), jnp.bfloat16)
    scratch = [pltpu.VMEM((N1, HALF), jnp.float32)] * 2
    inner = pl.pallas_call(
        inner_kernel,
        in_specs=[IN_VMEM] * 9,
        out_specs=IN_VMEM,
        out_shape=shape,
        scratch_shapes=scratch,
        compiler_params=params,
        cost_estimate=pl.CostEstimate(flops=14 * MACS, bytes_accessed=4 << 20, transcendentals=0),
        name="inner",
    )(recv, *consts)
    return pl.pallas_call(
        border_kernel,
        in_specs=[IN_VMEM] * 11,
        out_specs=IN_VMEM,
        out_shape=shape,
        input_output_aliases={0: 0},
        scratch_shapes=scratch,
        compiler_params=params,
        cost_estimate=pl.CostEstimate(flops=2 * MACS, bytes_accessed=3 << 20, transcendentals=0),
        name="border",
    )(inner, recv, border, *consts)


def pack_kernel(sl, tok, value, gate_in, piece, nyquist, out, turned):
    j = pl.program_id(0)

    @pl.when(j < N2 // LANES)
    def _():
        for row in range(ROW_T):
            v = value[row].astype(jnp.float32) * gate_in[row].astype(jnp.float32)
            v = v.astype(jnp.bfloat16).astype(jnp.float32)
            turned[pl.ds(row, LANES, stride=ROW_T), :] = v.T

    @pl.when(j == N2 // LANES)
    def _():
        mine = (tok[0] == 0) & (sl[0] % 4 == 0)
        for row in range(ROW_T):
            v = piece[0, row].astype(jnp.float32)
            if row == 0:
                edge = jnp.where(sl[0] // 4 == 0, v[0:1], nyquist[0, 0, 0:1].astype(jnp.float32))
                at_edge = (lax.broadcasted_iota(jnp.int32, v.shape, 0) == 0) & mine
                v = jnp.where(at_edge, 0.5 * edge, v)
            turned[pl.ds(row, LANES, stride=ROW_T), :] = v.T

    out[...] = turned[...].reshape(LANES, ROW_T, LANES).astype(jnp.bfloat16)


def pack(sl, tok, value, gate_in, filter_spectrum):
    last = N2 // LANES - 1
    block = pl.BlockSpec((ROW_T, LANES, LANES), lambda j, sl, tok: (0, jnp.minimum(j, last), 0))
    return pl.pallas_call(
        pack_kernel,
        grid_spec=pltpu.PrefetchScalarGridSpec(
            num_scalar_prefetch=2,
            grid=(WIDE // LANES,),
            in_specs=[
                block,
                block,
                pl.BlockSpec(
                    (1, ROW_T, LANES, LANES),
                    lambda j, sl, tok: (sl[0] // 4, (sl[0] // 2) % 2, sl[0] % 2, 0),
                ),
                pl.BlockSpec((1, 1, 8, LANES), lambda j, sl, tok: (0, 0, HALF // 8, 0)),
            ],
            out_specs=pl.BlockSpec((LANES, ROW_T, LANES), lambda j, sl, tok: (0, 0, j)),
            scratch_shapes=[pltpu.VMEM((LANES * ROW_T, LANES), jnp.float32)],
        ),
        out_shape=jax.ShapeDtypeStruct((LANES, ROW_T, WIDE), jnp.bfloat16),
        cost_estimate=pl.CostEstimate(flops=1 << 20, bytes_accessed=3 << 20, transcendentals=0),
        name="pack",
    )(sl, tok, value, gate_in, filter_spectrum, filter_spectrum)


def finish_kernel(back, value, gate_in, gate_out, skip, out, turned):
    turned[...] = back[...].astype(jnp.float32).reshape(LANES * ROW_T, LANES)
    for row in range(ROW_T):
        mixed = turned[pl.ds(row, LANES, stride=ROW_T), :].T
        gated = value[row].astype(jnp.float32) * gate_in[row].astype(jnp.float32)
        gated = gated.astype(jnp.bfloat16).astype(jnp.float32)
        res = gate_out[row].astype(jnp.float32) * (mixed + skip[...] * gated)
        out[row] = res.astype(jnp.bfloat16)


def finish(back, value, gate_in, gate_out, skip):
    block = pl.BlockSpec((ROW_T, LANES, LANES), lambda j: (0, j, 0))
    return pl.pallas_call(
        finish_kernel,
        grid=(N2 // LANES,),
        in_specs=[
            pl.BlockSpec((LANES, ROW_T, LANES), lambda j: (0, 0, j)),
            block,
            block,
            block,
            pl.BlockSpec((1, LANES), lambda j: (0, 0)),
        ],
        out_specs=block,
        out_shape=jax.ShapeDtypeStruct((ROW_T, N2, LANES), jnp.bfloat16),
        scratch_shapes=[pltpu.VMEM((LANES * ROW_T, LANES), jnp.float32)],
        cost_estimate=pl.CostEstimate(flops=1 << 20, bytes_accessed=5 << 20, transcendentals=0),
        name="finish",
    )(back, value, gate_in, gate_out, skip)


def shards(value, gate_in, gate_out, filter_spectrum, skip_gain):
    sl = lax.axis_index(("x", "core")).reshape(1)
    tok = lax.axis_index(("z", "yl")).reshape(1)
    cut = lambda a: a.reshape(ROW_T, N2, LANES)
    value = cut(value)
    gate_in = cut(gate_in)
    gate_out = cut(gate_out)
    send = pack(sl, tok, value, gate_in, filter_spectrum)
    recv = lax.all_to_all(send, GROUP, split_axis=0, concat_axis=0, tiled=True)
    recv = recv.reshape(SEGS, ROWS, WIDE)
    border = lax.ppermute(recv[SEGS - 1, :, :N2], "yh", [(0, 1)])
    mixed = convolve(recv, border, tables())
    back = lax.all_to_all(
        mixed.reshape(SEGS * 16, ROW_T, N2), GROUP, split_axis=0, concat_axis=0, tiled=True
    )
    result = finish(back, value, gate_in, gate_out, skip_gain.reshape(1, LANES))
    return result.reshape(-1, LANES)


def solution(mesh):
    fine = Mesh(mesh.devices.reshape(2, 4, 2, 8, 2), ALL)
    return jax.shard_map(
        shards,
        mesh=fine,
        in_specs=(
            P(ALL, None),
            P(ALL, None),
            P(ALL, None),
            P(None, ("z", "yl"), None, None),
            P(),
        ),
        out_specs=P(ALL, None),
        check_vma=False,
    )
```

```python
import functools
import math

import jax
import jax.numpy as jnp
import numpy as np
from jax import lax
from jax.experimental import pallas as pl
from jax.experimental.pallas import tpu as pltpu
from jax.sharding import Mesh, PartitionSpec as P

N1 = 256
N2 = 512
HALF = N2 // 2
ROWS = N1 // 2
FFT = N1 * N2
LANES = 128
SEGS = 8
ROW_T = 8
WIDE = N2 + LANES

ALL = ("yh", "x", "core", "z", "yl")
GROUP = ("x", "core", "z", "yl")


def trig(rows, cols, modulus):
    product = (rows[:, None].astype(np.int64) * cols[None, :]) % modulus
    angle = product.astype(np.float64) * (2.0 * math.pi / modulus)
    return np.cos(angle), np.sin(angle)


def tables():
    rh, t, row = np.meshgrid(np.arange(2), np.arange(16), np.arange(8), indexing="ij")
    k1 = (16 * t + 8 * rh + row).reshape(-1)
    n1 = np.arange(N1)
    n2 = np.arange(N2)
    k2 = np.arange(HALF)
    cos_one, sin_one = trig(k1, n1, N1)
    first = np.concatenate([cos_one, -sin_one], axis=0)
    cos_two, sin_two = trig(n2, k2, N2)
    tw_cos, tw_sin = trig(k1, n2, FFT)
    last = np.concatenate([cos_one.T[:ROWS], -sin_one.T[:ROWS]], axis=1)
    by_column = np.concatenate([first, cos_two, sin_two], axis=0)
    by_row = np.concatenate([cos_two.T, sin_two.T, last], axis=0)
    twiddles = np.concatenate([tw_cos, tw_sin], axis=0)
    return (
        np.asarray(by_column, dtype=jnp.bfloat16),
        np.asarray(by_row, dtype=jnp.bfloat16),
        np.asarray(twiddles, dtype=np.float32),
    )


def split_tables(by_column, by_row, twiddles):
    return (
        by_column.at[:N2],
        by_column.at[N2 : 2 * N2],
        by_column.at[2 * N2 :],
        by_row.at[:HALF],
        by_row.at[HALF:N2],
        twiddles.at[:N1],
        twiddles.at[N1:],
        by_row.at[N2:],
    )


def dot(a, b):
    return jnp.dot(a, b, preferred_element_type=jnp.float32)


def segments(pairs, outs, h_re, h_im, first, c2, s2, c3, s3, tc, ts, last):
    parity = lax.broadcasted_iota(jnp.int32, (1, N2), 1) % 2
    sign = (1 - 2 * parity).astype(jnp.float32)
    halves = []
    for cur, prev in pairs:
        a = dot(first[...], jnp.concatenate([cur, prev], axis=0))
        a_re = a[:N1]
        a_im = a[N1:]
        b_re = (a_re * tc[...] + a_im * ts[...]).astype(jnp.bfloat16)
        b_im = (a_im * tc[...] - a_re * ts[...]).astype(jnp.bfloat16)
        nyq = jnp.sum(a_re[0:1] * sign, axis=1, keepdims=True)
        halves.append((b_re, b_im, nyq))
    for (b_re, b_im, nyq), out in zip(halves, outs):
        x_re = dot(b_re, c2[...]) + dot(b_im, s2[...])
        x_im = dot(b_im, c2[...]) - dot(b_re, s2[...])
        hr = h_re[...]
        hi = h_im[...]
        z_re = (x_re * hr - x_im * hi).astype(jnp.bfloat16)
        z_im = (x_re * hi + x_im * hr).astype(jnp.bfloat16)
        p_re = dot(z_re, c3[...]) - dot(z_im, s3[...])
        p_im = dot(z_im, c3[...]) + dot(z_re, s3[...])
        q_re = (p_re * tc[...] - p_im * ts[...]).astype(jnp.bfloat16)
        q_im = (p_im * tc[...] + p_re * ts[...]).astype(jnp.bfloat16)
        total = dot(last[:, :N1], q_re) + dot(last[:, N1:], q_im)
        total = total + (nyq * h_im[0:1, 0:1]) * sign
        out[...] = (total * (2.0 / FFT)).astype(jnp.bfloat16)


def filter_parts(recv, h_re, h_im):
    for p, ref in enumerate((h_re, h_im)):
        for rh in range(2):
            for kh in range(2):
                ref[rh * ROWS : (rh + 1) * ROWS, kh * LANES : (kh + 1) * LANES] = recv[
                    p * 4 + rh * 2 + kh, :, N2:
                ].astype(jnp.float32)


def inner_kernel(recv, by_column, by_row, twiddles, out, h_re, h_im):
    filter_parts(recv, h_re, h_im)
    consts = (h_re, h_im) + split_tables(by_column, by_row, twiddles)

    def step(i, carry):
        s = 2 * i + 1
        segments(
            [(recv[s, :, :N2], recv[s - 1, :, :N2]), (recv[s + 1, :, :N2], recv[s, :, :N2])],
            [out.at[s], out.at[s + 1]],
            *consts,
        )
        return carry

    lax.fori_loop(0, (SEGS - 2) // 2, step, 0)


def border_kernel(yh, acc, recv, border, by_column, by_row, twiddles, out, h_re, h_im):
    filter_parts(recv, h_re, h_im)
    consts = (h_re, h_im) + split_tables(by_column, by_row, twiddles)
    before = jnp.where(yh[0] == 0, jnp.zeros_like(border), border[...])
    segments(
        [(recv[SEGS - 1, :, :N2], recv[SEGS - 2, :, :N2]), (recv[0, :, :N2], before)],
        [out.at[SEGS - 1], out.at[0]],
        *consts,
    )


MACS = 2 * N1 * N1 * N2 + 8 * N1 * N2 * HALF + ROWS * 2 * N1 * N2
IN_VMEM = pl.BlockSpec(memory_space=pltpu.VMEM)


def convolve(yh, recv, border, consts):
    params = pltpu.CompilerParams(vmem_limit_bytes=28 * 1024 * 1024)
    shape = jax.ShapeDtypeStruct((SEGS, ROWS, N2), jnp.bfloat16)
    scratch = [pltpu.VMEM((N1, HALF), jnp.float32)] * 2
    inner = pl.pallas_call(
        inner_kernel,
        in_specs=[IN_VMEM] * 4,
        out_specs=IN_VMEM,
        out_shape=shape,
        scratch_shapes=scratch,
        compiler_params=params,
        cost_estimate=pl.CostEstimate(flops=12 * MACS, bytes_accessed=4 << 20, transcendentals=0),
        name="inner",
    )(recv, *consts)
    return pl.pallas_call(
        border_kernel,
        in_specs=[pl.BlockSpec(memory_space=pltpu.SMEM)] + [IN_VMEM] * 6,
        out_specs=IN_VMEM,
        out_shape=shape,
        input_output_aliases={1: 0},
        scratch_shapes=scratch,
        compiler_params=params,
        cost_estimate=pl.CostEstimate(flops=4 * MACS, bytes_accessed=3 << 20, transcendentals=0),
        name="border",
    )(yh, inner, recv, border, *consts)


def edge_kernel(recv, out):
    out[...] = recv[SEGS - 1, :, :N2]


def edge(recv):
    return pl.pallas_call(
        edge_kernel,
        in_specs=[IN_VMEM],
        out_specs=IN_VMEM,
        out_shape=jax.ShapeDtypeStruct((ROWS, N2), jnp.bfloat16),
        compiler_params=pltpu.CompilerParams(vmem_limit_bytes=8 * 1024 * 1024),
        name="edge",
    )(recv)


CHUNKS = N2 // LANES
IN_SMEM = pl.BlockSpec(memory_space=pltpu.SMEM)
ANYWHERE = pl.BlockSpec(memory_space=pl.ANY)


def pack_kernel(sl, tok, value, gate_in, spectrum, out, vbuf, gbuf, pbuf, nbuf, turned, sems):
    part = sl[0] // 4
    rh = (sl[0] // 2) % 2
    kh = sl[0] % 2
    copies = []
    for j in range(CHUNKS):
        lanes = pl.ds(j * LANES, LANES)
        for i, (src, dst) in enumerate(((value, vbuf), (gate_in, gbuf))):
            copies.append(
                pltpu.make_async_copy(src.at[:, lanes, :], dst.at[:, lanes, :], sems.at[2 * j + i])
            )
    k_lanes = pl.ds(pl.multiple_of(kh * LANES, LANES), LANES)
    copies.append(
        pltpu.make_async_copy(
            spectrum.at[part, pl.ds(rh * ROW_T, ROW_T), k_lanes, :], pbuf, sems.at[2 * CHUNKS]
        )
    )
    copies.append(
        pltpu.make_async_copy(
            spectrum.at[0, 0, pl.ds(HALF, 8), :], nbuf, sems.at[2 * CHUNKS + 1]
        )
    )
    for copy in copies:
        copy.start()

    def place(j, row, v):
        turned[j % 2, pl.ds(row, LANES, stride=ROW_T), :] = v.T

    def write(j):
        lanes = slice(j * LANES, (j + 1) * LANES)
        out[:, :, lanes] = turned[j % 2].reshape(LANES, ROW_T, LANES).astype(jnp.bfloat16)

    for j in range(CHUNKS):
        copies[2 * j].wait()
        copies[2 * j + 1].wait()
        lanes = slice(j * LANES, (j + 1) * LANES)
        for row in range(ROW_T):
            v = vbuf[row, lanes].astype(jnp.float32) * gbuf[row, lanes].astype(jnp.float32)
            place(j, row, v.astype(jnp.bfloat16).astype(jnp.float32))
        write(j)
    copies[2 * CHUNKS].wait()
    copies[2 * CHUNKS + 1].wait()
    mine = (tok[0] == 0) & (sl[0] % 4 == 0)
    for row in range(ROW_T):
        v = pbuf[row].astype(jnp.float32)
        if row == 0:
            edge = jnp.where(part == 0, v[0:1], nbuf[0:1].astype(jnp.float32))
            at_edge = (lax.broadcasted_iota(jnp.int32, v.shape, 0) == 0) & mine
            v = jnp.where(at_edge, 0.5 * edge, v)
        place(CHUNKS, row, v)
    write(CHUNKS)


def pack(sl, tok, value, gate_in, filter_spectrum):
    return pl.pallas_call(
        pack_kernel,
        in_specs=[IN_SMEM, IN_SMEM, ANYWHERE, ANYWHERE, ANYWHERE],
        out_specs=IN_VMEM,
        out_shape=jax.ShapeDtypeStruct((LANES, ROW_T, WIDE), jnp.bfloat16),
        scratch_shapes=[
            pltpu.VMEM((ROW_T, N2, LANES), jnp.bfloat16),
            pltpu.VMEM((ROW_T, N2, LANES), jnp.bfloat16),
            pltpu.VMEM((ROW_T, LANES, LANES), jnp.bfloat16),
            pltpu.VMEM((8, LANES), jnp.bfloat16),
            pltpu.VMEM((2, LANES * ROW_T, LANES), jnp.float32),
            pltpu.SemaphoreType.DMA((2 * CHUNKS + 2,)),
        ],
        cost_estimate=pl.CostEstimate(flops=1 << 20, bytes_accessed=3 << 20, transcendentals=0),
        name="pack",
    )(sl, tok, value, gate_in, filter_spectrum)


def finish_kernel(back, value, gate_in, gate_out, skip, out, turned, obuf, sems):
    copies = []
    for j in range(CHUNKS):
        lanes = slice(j * LANES, (j + 1) * LANES)
        slot = j % 2
        turned[slot] = back[:, :, lanes].astype(jnp.float32).reshape(LANES * ROW_T, LANES)
        for row in range(ROW_T):
            mixed = turned[slot, pl.ds(row, LANES, stride=ROW_T), :].T
            gated = value[row, lanes].astype(jnp.float32) * gate_in[row, lanes].astype(jnp.float32)
            gated = gated.astype(jnp.bfloat16).astype(jnp.float32)
            res = gate_out[row, lanes].astype(jnp.float32) * (mixed + skip[...] * gated)
            obuf[row, lanes] = res.astype(jnp.bfloat16)
        where = pl.ds(j * LANES, LANES)
        copies.append(
            pltpu.make_async_copy(obuf.at[:, where, :], out.at[:, where, :], sems.at[j])
        )
        copies[-1].start()
    for copy in copies:
        copy.wait()


def finish(back, value, gate_in, gate_out, skip):
    return pl.pallas_call(
        finish_kernel,
        in_specs=[IN_VMEM] * 5,
        out_specs=ANYWHERE,
        out_shape=jax.ShapeDtypeStruct((ROW_T, N2, LANES), jnp.bfloat16),
        scratch_shapes=[
            pltpu.VMEM((2, LANES * ROW_T, LANES), jnp.float32),
            pltpu.VMEM((ROW_T, N2, LANES), jnp.bfloat16),
            pltpu.SemaphoreType.DMA((CHUNKS,)),
        ],
        compiler_params=pltpu.CompilerParams(vmem_limit_bytes=14 * 1024 * 1024),
        cost_estimate=pl.CostEstimate(flops=1 << 20, bytes_accessed=5 << 20, transcendentals=0),
        name="finish",
    )(back, value, gate_in, gate_out, skip)


def shards(value, gate_in, gate_out, filter_spectrum, skip_gain):
    sl = lax.axis_index(("x", "core")).reshape(1)
    tok = lax.axis_index(("z", "yl")).reshape(1)
    cut = lambda a: a.reshape(ROW_T, N2, LANES)
    value = cut(value)
    gate_in = cut(gate_in)
    gate_out = cut(gate_out)
    send = pack(sl, tok, value, gate_in, filter_spectrum)
    recv = lax.all_to_all(send, GROUP, split_axis=0, concat_axis=0, tiled=True)
    recv = recv.reshape(SEGS, ROWS, WIDE)
    border = lax.ppermute(edge(recv), "yh", [(0, 1), (1, 0)])
    mixed = convolve(lax.axis_index("yh").reshape(1), recv, border, tables())
    back = lax.all_to_all(
        mixed.reshape(SEGS * 16, ROW_T, N2), GROUP, split_axis=0, concat_axis=0, tiled=True
    )
    result = finish(back, value, gate_in, gate_out, skip_gain.reshape(1, LANES))
    return result.reshape(-1, LANES)


def solution(mesh):
    fine = Mesh(mesh.devices.reshape(2, 4, 2, 8, 2), ALL)
    return jax.shard_map(
        shards,
        mesh=fine,
        in_specs=(
            P(ALL, None),
            P(ALL, None),
            P(ALL, None),
            P(None, ("z", "yl"), None, None),
            P(),
        ),
        out_specs=P(ALL, None),
        check_vma=False,
    )
```

```python
import functools
import math

import jax
import jax.numpy as jnp
import numpy as np
from jax import lax
from jax.experimental import pallas as pl
from jax.experimental.pallas import tpu as pltpu
from jax.sharding import Mesh, PartitionSpec as P

N1 = 256
N2 = 512
HALF = N2 // 2
ROWS = N1 // 2
FFT = N1 * N2
LANES = 128
SEGS = 8
ROW_T = 8
WIDE = N2 + LANES

ALL = ("yh", "x", "core", "z", "yl")
GROUP = ("x", "core", "z", "yl")


def trig(rows, cols, modulus):
    product = (rows[:, None].astype(np.int64) * cols[None, :]) % modulus
    angle = product.astype(np.float64) * (2.0 * math.pi / modulus)
    return np.cos(angle), np.sin(angle)


def tables():
    rh, t, row = np.meshgrid(np.arange(2), np.arange(16), np.arange(8), indexing="ij")
    k1 = (16 * t + 8 * rh + row).reshape(-1)
    n1 = np.arange(N1)
    n2 = np.arange(N2)
    k2 = np.arange(HALF)
    cos_one, sin_one = trig(k1, n1, N1)
    first = np.concatenate([cos_one, -sin_one], axis=0)
    cos_two, sin_two = trig(n2, k2, N2)
    tw_cos, tw_sin = trig(k1, n2, FFT)
    last = np.concatenate([cos_one.T[:ROWS], -sin_one.T[:ROWS]], axis=1)
    by_column = np.concatenate([first, cos_two, sin_two], axis=0)
    by_row = np.concatenate([cos_two.T, sin_two.T, last], axis=0)
    twiddles = np.concatenate([tw_cos, tw_sin], axis=0)
    return (
        np.asarray(by_column, dtype=jnp.bfloat16),
        np.asarray(by_row, dtype=jnp.bfloat16),
        np.asarray(twiddles, dtype=np.float32),
    )


def split_tables(by_column, by_row, twiddles):
    return (
        by_column.at[:N2],
        by_column.at[N2 : 2 * N2],
        by_column.at[2 * N2 :],
        by_row.at[:HALF],
        by_row.at[HALF:N2],
        twiddles.at[:N1],
        twiddles.at[N1:],
        by_row.at[N2:],
    )


def dot(a, b):
    return jnp.dot(a, b, preferred_element_type=jnp.float32)


def segments(pairs, outs, h_re, h_im, first, c2, s2, c3, s3, tc, ts, last):
    parity = lax.broadcasted_iota(jnp.int32, (1, N2), 1) % 2
    sign = (1 - 2 * parity).astype(jnp.float32)
    b_re = []
    b_im = []
    nyq = []
    for cur, prev in pairs:
        a = dot(first[...], jnp.concatenate([cur, prev], axis=0))
        a_re = a[:N1]
        a_im = a[N1:]
        b_re.append((a_re * tc[...] + a_im * ts[...]).astype(jnp.bfloat16))
        b_im.append((a_im * tc[...] - a_re * ts[...]).astype(jnp.bfloat16))
        nyq.append(jnp.sum(a_re[0:1] * sign, axis=1, keepdims=True))
    b_re = jnp.concatenate(b_re, axis=0)
    b_im = jnp.concatenate(b_im, axis=0)
    x_re = dot(b_re, c2[...]) + dot(b_im, s2[...])
    x_im = dot(b_im, c2[...]) - dot(b_re, s2[...])
    z_re = []
    z_im = []
    for i in range(len(pairs)):
        rows = slice(i * N1, (i + 1) * N1)
        hr = h_re[...]
        hi = h_im[...]
        z_re.append((x_re[rows] * hr - x_im[rows] * hi).astype(jnp.bfloat16))
        z_im.append((x_re[rows] * hi + x_im[rows] * hr).astype(jnp.bfloat16))
    z_re = jnp.concatenate(z_re, axis=0)
    z_im = jnp.concatenate(z_im, axis=0)
    p_re = dot(z_re, c3[...]) - dot(z_im, s3[...])
    p_im = dot(z_im, c3[...]) + dot(z_re, s3[...])
    for i, out in enumerate(outs):
        rows = slice(i * N1, (i + 1) * N1)
        q_re = (p_re[rows] * tc[...] - p_im[rows] * ts[...]).astype(jnp.bfloat16)
        q_im = (p_im[rows] * tc[...] + p_re[rows] * ts[...]).astype(jnp.bfloat16)
        total = dot(last[:, :N1], q_re) + dot(last[:, N1:], q_im)
        total = total + (nyq[i] * h_im[0:1, 0:1]) * sign
        out[...] = (total * (2.0 / FFT)).astype(jnp.bfloat16)


def filter_parts(recv, h_re, h_im):
    for p, ref in enumerate((h_re, h_im)):
        for rh in range(2):
            for kh in range(2):
                ref[rh * ROWS : (rh + 1) * ROWS, kh * LANES : (kh + 1) * LANES] = recv[
                    p * 4 + rh * 2 + kh, :, N2:
                ].astype(jnp.float32)


def inner_kernel(recv, by_column, by_row, twiddles, out, h_re, h_im):
    filter_parts(recv, h_re, h_im)
    consts = (h_re, h_im) + split_tables(by_column, by_row, twiddles)

    def step(i, carry):
        s = 2 * i + 1
        segments(
            [(recv[s, :, :N2], recv[s - 1, :, :N2]), (recv[s + 1, :, :N2], recv[s, :, :N2])],
            [out.at[s], out.at[s + 1]],
            *consts,
        )
        return carry

    lax.fori_loop(0, (SEGS - 2) // 2, step, 0, unroll=True)


def border_kernel(yh, acc, recv, border, by_column, by_row, twiddles, out, h_re, h_im):
    filter_parts(recv, h_re, h_im)
    consts = (h_re, h_im) + split_tables(by_column, by_row, twiddles)
    before = jnp.where(yh[0] == 0, jnp.zeros_like(border), border[...])
    segments(
        [(recv[SEGS - 1, :, :N2], recv[SEGS - 2, :, :N2]), (recv[0, :, :N2], before)],
        [out.at[SEGS - 1], out.at[0]],
        *consts,
    )


MACS = 2 * N1 * N1 * N2 + 8 * N1 * N2 * HALF + ROWS * 2 * N1 * N2
IN_VMEM = pl.BlockSpec(memory_space=pltpu.VMEM)


def convolve(yh, recv, border, consts):
    params = pltpu.CompilerParams(vmem_limit_bytes=28 * 1024 * 1024)
    shape = jax.ShapeDtypeStruct((SEGS, ROWS, N2), jnp.bfloat16)
    scratch = [pltpu.VMEM((N1, HALF), jnp.float32)] * 2
    inner = pl.pallas_call(
        inner_kernel,
        in_specs=[IN_VMEM] * 4,
        out_specs=IN_VMEM,
        out_shape=shape,
        scratch_shapes=scratch,
        compiler_params=params,
        cost_estimate=pl.CostEstimate(flops=12 * MACS, bytes_accessed=4 << 20, transcendentals=0),
        name="inner",
    )(recv, *consts)
    return pl.pallas_call(
        border_kernel,
        in_specs=[pl.BlockSpec(memory_space=pltpu.SMEM)] + [IN_VMEM] * 6,
        out_specs=IN_VMEM,
        out_shape=shape,
        input_output_aliases={1: 0},
        scratch_shapes=scratch,
        compiler_params=params,
        cost_estimate=pl.CostEstimate(flops=4 * MACS, bytes_accessed=3 << 20, transcendentals=0),
        name="border",
    )(yh, inner, recv, border, *consts)


def hold_kernel(table, out):
    out[...] = table[...]


def hold(table):
    return pl.pallas_call(
        hold_kernel,
        in_specs=[IN_VMEM],
        out_specs=IN_VMEM,
        out_shape=jax.ShapeDtypeStruct(table.shape, table.dtype),
        compiler_params=pltpu.CompilerParams(vmem_limit_bytes=8 * 1024 * 1024),
        cost_estimate=pl.CostEstimate(flops=1 << 20, bytes_accessed=1 << 20, transcendentals=0),
        name="hold",
    )(table)


def edge_kernel(recv, out):
    out[...] = recv[SEGS - 1, :, :N2]


def edge(recv):
    return pl.pallas_call(
        edge_kernel,
        in_specs=[IN_VMEM],
        out_specs=IN_VMEM,
        out_shape=jax.ShapeDtypeStruct((ROWS, N2), jnp.bfloat16),
        compiler_params=pltpu.CompilerParams(vmem_limit_bytes=8 * 1024 * 1024),
        name="edge",
    )(recv)


CHUNKS = N2 // LANES
IN_SMEM = pl.BlockSpec(memory_space=pltpu.SMEM)
ANYWHERE = pl.BlockSpec(memory_space=pl.ANY)


def pack_kernel(sl, tok, value, gate_in, spectrum, out, vbuf, gbuf, pbuf, nbuf, turned, sems):
    part = sl[0] // 4
    rh = (sl[0] // 2) % 2
    kh = sl[0] % 2
    copies = []
    for j in range(CHUNKS):
        lanes = pl.ds(j * LANES, LANES)
        for i, (src, dst) in enumerate(((value, vbuf), (gate_in, gbuf))):
            copies.append(
                pltpu.make_async_copy(src.at[:, lanes, :], dst.at[:, lanes, :], sems.at[2 * j + i])
            )
    k_lanes = pl.ds(pl.multiple_of(kh * LANES, LANES), LANES)
    copies.append(
        pltpu.make_async_copy(
            spectrum.at[part, pl.ds(rh * ROW_T, ROW_T), k_lanes, :], pbuf, sems.at[2 * CHUNKS]
        )
    )
    copies.append(
        pltpu.make_async_copy(
            spectrum.at[0, 0, pl.ds(HALF, 8), :], nbuf, sems.at[2 * CHUNKS + 1]
        )
    )
    for copy in copies:
        copy.start()

    def place(j, row, v):
        turned[j % 2, pl.ds(row, LANES, stride=ROW_T), :] = v.T

    def write(j):
        lanes = slice(j * LANES, (j + 1) * LANES)
        out[:, :, lanes] = turned[j % 2].reshape(LANES, ROW_T, LANES).astype(jnp.bfloat16)

    for j in range(CHUNKS):
        copies[2 * j].wait()
        copies[2 * j + 1].wait()
        lanes = slice(j * LANES, (j + 1) * LANES)
        for row in range(ROW_T):
            v = vbuf[row, lanes].astype(jnp.float32) * gbuf[row, lanes].astype(jnp.float32)
            place(j, row, v.astype(jnp.bfloat16).astype(jnp.float32))
        write(j)
    copies[2 * CHUNKS].wait()
    copies[2 * CHUNKS + 1].wait()
    mine = (tok[0] == 0) & (sl[0] % 4 == 0)
    for row in range(ROW_T):
        v = pbuf[row].astype(jnp.float32)
        if row == 0:
            edge = jnp.where(part == 0, v[0:1], nbuf[0:1].astype(jnp.float32))
            at_edge = (lax.broadcasted_iota(jnp.int32, v.shape, 0) == 0) & mine
            v = jnp.where(at_edge, 0.5 * edge, v)
        place(CHUNKS, row, v)
    write(CHUNKS)


def pack(sl, tok, value, gate_in, filter_spectrum):
    return pl.pallas_call(
        pack_kernel,
        in_specs=[IN_SMEM, IN_SMEM, ANYWHERE, ANYWHERE, ANYWHERE],
        out_specs=IN_VMEM,
        out_shape=jax.ShapeDtypeStruct((LANES, ROW_T, WIDE), jnp.bfloat16),
        scratch_shapes=[
            pltpu.VMEM((ROW_T, N2, LANES), jnp.bfloat16),
            pltpu.VMEM((ROW_T, N2, LANES), jnp.bfloat16),
            pltpu.VMEM((ROW_T, LANES, LANES), jnp.bfloat16),
            pltpu.VMEM((8, LANES), jnp.bfloat16),
            pltpu.VMEM((2, LANES * ROW_T, LANES), jnp.float32),
            pltpu.SemaphoreType.DMA((2 * CHUNKS + 2,)),
        ],
        compiler_params=pltpu.CompilerParams(),
        cost_estimate=pl.CostEstimate(flops=1 << 20, bytes_accessed=3 << 20, transcendentals=0),
        name="pack",
    )(sl, tok, value, gate_in, filter_spectrum)


def finish_kernel(back, value, gate_in, gate_out, skip, out, turned, obuf, sems):
    copies = []
    for j in range(CHUNKS):
        lanes = slice(j * LANES, (j + 1) * LANES)
        slot = j % 2
        turned[slot] = back[:, :, lanes].astype(jnp.float32).reshape(LANES * ROW_T, LANES)
        for row in range(ROW_T):
            mixed = turned[slot, pl.ds(row, LANES, stride=ROW_T), :].T
            gated = value[row, lanes].astype(jnp.float32) * gate_in[row, lanes].astype(jnp.float32)
            gated = gated.astype(jnp.bfloat16).astype(jnp.float32)
            res = gate_out[row, lanes].astype(jnp.float32) * (mixed + skip[...] * gated)
            obuf[row, lanes] = res.astype(jnp.bfloat16)
        where = pl.ds(j * LANES, LANES)
        copies.append(
            pltpu.make_async_copy(obuf.at[:, where, :], out.at[:, where, :], sems.at[j])
        )
        copies[-1].start()
    for copy in copies:
        copy.wait()


def finish(back, value, gate_in, gate_out, skip):
    return pl.pallas_call(
        finish_kernel,
        in_specs=[IN_VMEM] * 5,
        out_specs=ANYWHERE,
        out_shape=jax.ShapeDtypeStruct((ROW_T, N2, LANES), jnp.bfloat16),
        scratch_shapes=[
            pltpu.VMEM((2, LANES * ROW_T, LANES), jnp.float32),
            pltpu.VMEM((ROW_T, N2, LANES), jnp.bfloat16),
            pltpu.SemaphoreType.DMA((CHUNKS,)),
        ],
        compiler_params=pltpu.CompilerParams(
            vmem_limit_bytes=14 * 1024 * 1024
        ),
        cost_estimate=pl.CostEstimate(flops=1 << 20, bytes_accessed=5 << 20, transcendentals=0),
        name="finish",
    )(back, value, gate_in, gate_out, skip)


def shards(value, gate_in, gate_out, filter_spectrum, skip_gain):
    sl = lax.axis_index(("x", "core")).reshape(1)
    tok = lax.axis_index(("z", "yl")).reshape(1)
    cut = lambda a: a.reshape(ROW_T, N2, LANES)
    value = cut(value)
    gate_in = cut(gate_in)
    gate_out = cut(gate_out)
    send = pack(sl, tok, value, gate_in, filter_spectrum)
    by_column, by_row, twiddles = tables()
    send, by_row = lax.optimization_barrier((send, by_row))
    recv = lax.all_to_all(send, GROUP, split_axis=0, concat_axis=0, tiled=True)
    recv = recv.reshape(SEGS, ROWS, WIDE)
    border = lax.ppermute(edge(recv), "yh", [(0, 1), (1, 0)])
    by_row = hold(by_row)
    mixed = convolve(lax.axis_index("yh").reshape(1), recv, border, (by_column, by_row, twiddles))
    back = lax.all_to_all(
        mixed.reshape(SEGS * 16, ROW_T, N2), GROUP, split_axis=0, concat_axis=0, tiled=True
    )
    result = finish(back, value, gate_in, gate_out, skip_gain.reshape(1, LANES))
    return result.reshape(-1, LANES)


def solution(mesh):
    fine = Mesh(mesh.devices.reshape(2, 4, 2, 8, 2), ALL)
    return jax.shard_map(
        shards,
        mesh=fine,
        in_specs=(
            P(ALL, None),
            P(ALL, None),
            P(ALL, None),
            P(None, ("z", "yl"), None, None),
            P(),
        ),
        out_specs=P(ALL, None),
        check_vma=False,
    )
```

```python
import functools
import math

import jax
import jax.numpy as jnp
import numpy as np
from jax import lax
from jax.experimental import pallas as pl
from jax.experimental.pallas import tpu as pltpu
from jax.sharding import Mesh, PartitionSpec as P

N1 = 256
N2 = 512
HALF = N2 // 2
ROWS = N1 // 2
FFT = N1 * N2
LANES = 128
SEGS = 8
ROW_T = 8
WIDE = N2 + LANES

ALL = ("yh", "x", "core", "z", "yl")
GROUP = ("x", "core", "z", "yl")


def trig(rows, cols, modulus):
    product = (rows[:, None].astype(np.int64) * cols[None, :]) % modulus
    angle = product.astype(np.float64) * (2.0 * math.pi / modulus)
    return np.cos(angle), np.sin(angle)


def tables():
    rh, t, row = np.meshgrid(np.arange(2), np.arange(16), np.arange(8), indexing="ij")
    k1 = (16 * t + 8 * rh + row).reshape(-1)
    n1 = np.arange(N1)
    n2 = np.arange(N2)
    k2 = np.arange(HALF)
    cos_one, sin_one = trig(k1, n1, N1)
    first = np.concatenate([cos_one, -sin_one], axis=0)
    cos_two, sin_two = trig(n2, k2, N2)
    tw_cos, tw_sin = trig(k1, n2, FFT)
    last = np.concatenate([cos_one.T[:ROWS], -sin_one.T[:ROWS]], axis=1)
    by_column = np.concatenate([first, cos_two, sin_two], axis=0)
    by_row = np.concatenate([cos_two.T, sin_two.T, last], axis=0)
    twiddles = np.concatenate([tw_cos, tw_sin], axis=0)
    return (
        np.asarray(by_column, dtype=jnp.bfloat16),
        np.asarray(by_row, dtype=jnp.bfloat16),
        np.asarray(twiddles, dtype=np.float32),
    )


def split_tables(by_column, by_row, twiddles):
    return (
        by_column.at[:N2],
        by_column.at[N2 : 2 * N2],
        by_column.at[2 * N2 :],
        by_row.at[:HALF],
        by_row.at[HALF:N2],
        twiddles.at[:N1],
        twiddles.at[N1:],
        by_row.at[N2:],
    )


def dot(a, b):
    return jnp.dot(a, b, preferred_element_type=jnp.float32)


def segments(pairs, outs, h_re, h_im, first, c2, s2, c3, s3, tc, ts, last):
    parity = lax.broadcasted_iota(jnp.int32, (1, N2), 1) % 2
    sign = (1 - 2 * parity).astype(jnp.float32)
    b_re = []
    b_im = []
    nyq = []
    for cur, prev in pairs:
        a = dot(first[...], jnp.concatenate([cur, prev], axis=0))
        a_re = a[:N1]
        a_im = a[N1:]
        b_re.append((a_re * tc[...] + a_im * ts[...]).astype(jnp.bfloat16))
        b_im.append((a_im * tc[...] - a_re * ts[...]).astype(jnp.bfloat16))
        nyq.append(jnp.sum(a_re[0:1] * sign, axis=1, keepdims=True))
    b_re = jnp.concatenate(b_re, axis=0)
    b_im = jnp.concatenate(b_im, axis=0)
    x_re = dot(b_re, c2[...]) + dot(b_im, s2[...])
    x_im = dot(b_im, c2[...]) - dot(b_re, s2[...])
    z_re = []
    z_im = []
    for i in range(len(pairs)):
        rows = slice(i * N1, (i + 1) * N1)
        hr = h_re[...]
        hi = h_im[...]
        z_re.append((x_re[rows] * hr - x_im[rows] * hi).astype(jnp.bfloat16))
        z_im.append((x_re[rows] * hi + x_im[rows] * hr).astype(jnp.bfloat16))
    z_re = jnp.concatenate(z_re, axis=0)
    z_im = jnp.concatenate(z_im, axis=0)
    p_re = dot(z_re, c3[...]) - dot(z_im, s3[...])
    p_im = dot(z_im, c3[...]) + dot(z_re, s3[...])
    for i, out in enumerate(outs):
        rows = slice(i * N1, (i + 1) * N1)
        q_re = (p_re[rows] * tc[...] - p_im[rows] * ts[...]).astype(jnp.bfloat16)
        q_im = (p_im[rows] * tc[...] + p_re[rows] * ts[...]).astype(jnp.bfloat16)
        total = dot(last[:, :N1], q_re) + dot(last[:, N1:], q_im)
        total = total + (nyq[i] * h_im[0:1, 0:1]) * sign
        out[...] = (total * (2.0 / FFT)).astype(jnp.bfloat16)


def filter_parts(recv, h_re, h_im):
    for p, ref in enumerate((h_re, h_im)):
        for rh in range(2):
            for kh in range(2):
                ref[rh * ROWS : (rh + 1) * ROWS, kh * LANES : (kh + 1) * LANES] = recv[
                    p * 4 + rh * 2 + kh, :, N2:
                ].astype(jnp.float32)


def inner_kernel(recv, by_column, by_row, twiddles, out, h_re, h_im):
    filter_parts(recv, h_re, h_im)
    consts = (h_re, h_im) + split_tables(by_column, by_row, twiddles)

    def step(i, carry):
        s = 2 * i + 1
        segments(
            [(recv[s, :, :N2], recv[s - 1, :, :N2]), (recv[s + 1, :, :N2], recv[s, :, :N2])],
            [out.at[s], out.at[s + 1]],
            *consts,
        )
        return carry

    lax.fori_loop(0, (SEGS - 2) // 2, step, 0, unroll=True)


def border_kernel(yh, acc, recv, border, by_column, by_row, twiddles, out, h_re, h_im):
    filter_parts(recv, h_re, h_im)
    consts = (h_re, h_im) + split_tables(by_column, by_row, twiddles)
    before = jnp.where(yh[0] == 0, jnp.zeros_like(border), border[...])
    segments(
        [(recv[SEGS - 1, :, :N2], recv[SEGS - 2, :, :N2]), (recv[0, :, :N2], before)],
        [out.at[SEGS - 1], out.at[0]],
        *consts,
    )


MACS = 2 * N1 * N1 * N2 + 8 * N1 * N2 * HALF + ROWS * 2 * N1 * N2
IN_VMEM = pl.BlockSpec(memory_space=pltpu.VMEM)


def convolve(yh, recv, border, consts):
    params = pltpu.CompilerParams(vmem_limit_bytes=28 * 1024 * 1024)
    shape = jax.ShapeDtypeStruct((SEGS, ROWS, N2), jnp.bfloat16)
    scratch = [pltpu.VMEM((N1, HALF), jnp.float32)] * 2
    inner = pl.pallas_call(
        inner_kernel,
        in_specs=[IN_VMEM] * 4,
        out_specs=IN_VMEM,
        out_shape=shape,
        scratch_shapes=scratch,
        compiler_params=params,
        cost_estimate=pl.CostEstimate(flops=12 * MACS, bytes_accessed=4 << 20, transcendentals=0),
        name="inner",
    )(recv, *consts)
    return pl.pallas_call(
        border_kernel,
        in_specs=[pl.BlockSpec(memory_space=pltpu.SMEM)] + [IN_VMEM] * 6,
        out_specs=IN_VMEM,
        out_shape=shape,
        input_output_aliases={1: 0},
        scratch_shapes=scratch,
        compiler_params=params,
        cost_estimate=pl.CostEstimate(flops=4 * MACS, bytes_accessed=3 << 20, transcendentals=0),
        name="border",
    )(yh, inner, recv, border, *consts)


def hold_kernel(table, out):
    out[...] = table[...]


def hold(table):
    return pl.pallas_call(
        hold_kernel,
        in_specs=[IN_VMEM],
        out_specs=IN_VMEM,
        out_shape=jax.ShapeDtypeStruct(table.shape, table.dtype),
        compiler_params=pltpu.CompilerParams(vmem_limit_bytes=8 * 1024 * 1024),
        cost_estimate=pl.CostEstimate(flops=1 << 20, bytes_accessed=1 << 20, transcendentals=0),
        name="hold",
    )(table)


def edge_kernel(recv, out):
    out[...] = recv[SEGS - 1, :, :N2]


def edge(recv):
    return pl.pallas_call(
        edge_kernel,
        in_specs=[IN_VMEM],
        out_specs=IN_VMEM,
        out_shape=jax.ShapeDtypeStruct((ROWS, N2), jnp.bfloat16),
        compiler_params=pltpu.CompilerParams(vmem_limit_bytes=8 * 1024 * 1024),
        name="edge",
    )(recv)


CHUNKS = N2 // LANES
IN_SMEM = pl.BlockSpec(memory_space=pltpu.SMEM)
ANYWHERE = pl.BlockSpec(memory_space=pl.ANY)


def pack_kernel(sl, tok, value, gate_in, spectrum, out, vbuf, gbuf, pbuf, nbuf, turned, sems):
    part = sl[0] // 4
    rh = (sl[0] // 2) % 2
    kh = sl[0] % 2
    k_lanes = pl.ds(pl.multiple_of(kh * LANES, LANES), LANES)
    piece = pltpu.make_async_copy(
        spectrum.at[part, pl.ds(rh * ROW_T, ROW_T), k_lanes, :], pbuf, sems.at[2 * CHUNKS]
    )
    nyquist = pltpu.make_async_copy(
        spectrum.at[0, 0, pl.ds(HALF, 8), :], nbuf, sems.at[2 * CHUNKS + 1]
    )
    piece.start()
    nyquist.start()
    copies = []
    for j in range(CHUNKS):
        lanes = pl.ds(j * LANES, LANES)
        for i, (src, dst) in enumerate(((value, vbuf), (gate_in, gbuf))):
            copies.append(
                pltpu.make_async_copy(src.at[:, lanes, :], dst.at[:, lanes, :], sems.at[2 * j + i])
            )
            copies[-1].start()

    def place(j, row, v):
        turned[j % 2, pl.ds(row, LANES, stride=ROW_T), :] = v.T

    def write(j):
        lanes = slice(j * LANES, (j + 1) * LANES)
        out[:, :, lanes] = turned[j % 2].reshape(LANES, ROW_T, LANES).astype(jnp.bfloat16)

    piece.wait()
    nyquist.wait()
    mine = (tok[0] == 0) & (sl[0] % 4 == 0)
    for row in range(ROW_T):
        v = pbuf[row].astype(jnp.float32)
        if row == 0:
            edge = jnp.where(part == 0, v[0:1], nbuf[0:1].astype(jnp.float32))
            at_edge = (lax.broadcasted_iota(jnp.int32, v.shape, 0) == 0) & mine
            v = jnp.where(at_edge, 0.5 * edge, v)
        place(CHUNKS, row, v)
    write(CHUNKS)
    for j in range(CHUNKS):
        copies[2 * j].wait()
        copies[2 * j + 1].wait()
        lanes = slice(j * LANES, (j + 1) * LANES)
        for row in range(ROW_T):
            v = vbuf[row, lanes].astype(jnp.float32) * gbuf[row, lanes].astype(jnp.float32)
            place(j + 1, row, v.astype(jnp.bfloat16).astype(jnp.float32))
        out[:, :, lanes] = turned[(j + 1) % 2].reshape(LANES, ROW_T, LANES).astype(jnp.bfloat16)


def pack(sl, tok, value, gate_in, filter_spectrum):
    return pl.pallas_call(
        pack_kernel,
        in_specs=[IN_SMEM, IN_SMEM, ANYWHERE, ANYWHERE, ANYWHERE],
        out_specs=IN_VMEM,
        out_shape=jax.ShapeDtypeStruct((LANES, ROW_T, WIDE), jnp.bfloat16),
        scratch_shapes=[
            pltpu.VMEM((ROW_T, N2, LANES), jnp.bfloat16),
            pltpu.VMEM((ROW_T, N2, LANES), jnp.bfloat16),
            pltpu.VMEM((ROW_T, LANES, LANES), jnp.bfloat16),
            pltpu.VMEM((8, LANES), jnp.bfloat16),
            pltpu.VMEM((2, LANES * ROW_T, LANES), jnp.float32),
            pltpu.SemaphoreType.DMA((2 * CHUNKS + 2,)),
        ],
        cost_estimate=pl.CostEstimate(flops=1 << 20, bytes_accessed=3 << 20, transcendentals=0),
        name="pack",
    )(sl, tok, value, gate_in, filter_spectrum)


def finish_kernel(back, value, gate_in, gate_out, skip, out, turned, obuf, sems):
    copies = []
    for j in range(CHUNKS):
        lanes = slice(j * LANES, (j + 1) * LANES)
        slot = j % 2
        turned[slot] = back[:, :, lanes].astype(jnp.float32).reshape(LANES * ROW_T, LANES)
        for row in range(ROW_T):
            mixed = turned[slot, pl.ds(row, LANES, stride=ROW_T), :].T
            gated = value[row, lanes].astype(jnp.float32) * gate_in[row, lanes].astype(jnp.float32)
            gated = gated.astype(jnp.bfloat16).astype(jnp.float32)
            res = gate_out[row, lanes].astype(jnp.float32) * (mixed + skip[...] * gated)
            obuf[row, lanes] = res.astype(jnp.bfloat16)
        where = pl.ds(j * LANES, LANES)
        copies.append(
            pltpu.make_async_copy(obuf.at[:, where, :], out.at[:, where, :], sems.at[j])
        )
        copies[-1].start()
    for copy in copies:
        copy.wait()


def finish(back, value, gate_in, gate_out, skip):
    return pl.pallas_call(
        finish_kernel,
        in_specs=[IN_VMEM] * 5,
        out_specs=ANYWHERE,
        out_shape=jax.ShapeDtypeStruct((ROW_T, N2, LANES), jnp.bfloat16),
        scratch_shapes=[
            pltpu.VMEM((2, LANES * ROW_T, LANES), jnp.float32),
            pltpu.VMEM((ROW_T, N2, LANES), jnp.bfloat16),
            pltpu.SemaphoreType.DMA((CHUNKS,)),
        ],
        compiler_params=pltpu.CompilerParams(
            vmem_limit_bytes=14 * 1024 * 1024
        ),
        cost_estimate=pl.CostEstimate(flops=1 << 20, bytes_accessed=5 << 20, transcendentals=0),
        name="finish",
    )(back, value, gate_in, gate_out, skip)


def shards(value, gate_in, gate_out, filter_spectrum, skip_gain):
    sl = lax.axis_index(("x", "core")).reshape(1)
    tok = lax.axis_index(("z", "yl")).reshape(1)
    cut = lambda a: a.reshape(ROW_T, N2, LANES)
    value = cut(value)
    gate_in = cut(gate_in)
    gate_out = cut(gate_out)
    send = pack(sl, tok, value, gate_in, filter_spectrum)
    by_column, by_row, twiddles = tables()
    send, by_row = lax.optimization_barrier((send, by_row))
    recv = lax.all_to_all(send, GROUP, split_axis=0, concat_axis=0, tiled=True)
    recv = recv.reshape(SEGS, ROWS, WIDE)
    border = lax.ppermute(edge(recv), "yh", [(0, 1), (1, 0)])
    by_row = hold(by_row)
    mixed = convolve(lax.axis_index("yh").reshape(1), recv, border, (by_column, by_row, twiddles))
    back = lax.all_to_all(
        mixed.reshape(SEGS * 16, ROW_T, N2), GROUP, split_axis=0, concat_axis=0, tiled=True
    )
    result = finish(back, value, gate_in, gate_out, skip_gain.reshape(1, LANES))
    return result.reshape(-1, LANES)


def solution(mesh):
    fine = Mesh(mesh.devices.reshape(2, 4, 2, 8, 2), ALL)
    return jax.shard_map(
        shards,
        mesh=fine,
        in_specs=(
            P(ALL, None),
            P(ALL, None),
            P(ALL, None),
            P(None, ("z", "yl"), None, None),
            P(),
        ),
        out_specs=P(ALL, None),
        check_vma=False,
    )
```

```python
import functools
import math

import jax
import jax.numpy as jnp
import numpy as np
from jax import lax
from jax.experimental import pallas as pl
from jax.experimental.pallas import tpu as pltpu
from jax.sharding import Mesh, PartitionSpec as P

N1 = 256
N2 = 512
HALF = N2 // 2
ROWS = N1 // 2
FFT = N1 * N2
LANES = 128
SEGS = 8
ROW_T = 8
WIDE = N2 + LANES

ALL = ("yh", "x", "core", "z", "yl")
GROUP = ("x", "core", "z", "yl")


def trig(rows, cols, modulus):
    product = (rows[:, None].astype(np.int64) * cols[None, :]) % modulus
    angle = product.astype(np.float64) * (2.0 * math.pi / modulus)
    return np.cos(angle), np.sin(angle)


def tables():
    rh, t, row = np.meshgrid(np.arange(2), np.arange(16), np.arange(8), indexing="ij")
    k1 = (16 * t + 8 * rh + row).reshape(-1)
    n1 = np.arange(N1)
    n2 = np.arange(N2)
    k2 = np.arange(HALF)
    cos_one, sin_one = trig(k1, n1, N1)
    first = np.concatenate([cos_one, -sin_one], axis=0)
    cos_two, sin_two = trig(n2, k2, N2)
    tw_cos, tw_sin = trig(k1, n2, FFT)
    last = np.concatenate([cos_one.T[:ROWS], -sin_one.T[:ROWS]], axis=1)
    by_column = np.concatenate([first, cos_two, sin_two], axis=0)
    by_row = np.concatenate([cos_two.T, sin_two.T, last], axis=0)
    twiddles = np.concatenate([tw_cos, tw_sin], axis=0)
    return (
        np.asarray(by_column, dtype=jnp.bfloat16),
        np.asarray(by_row, dtype=jnp.bfloat16),
        np.asarray(twiddles, dtype=np.float32),
    )


def split_tables(by_column, by_row, twiddles):
    return (
        by_column.at[:N2],
        by_column.at[N2 : 2 * N2],
        by_column.at[2 * N2 :],
        by_row.at[:HALF],
        by_row.at[HALF:N2],
        twiddles.at[:N1],
        twiddles.at[N1:],
        by_row.at[N2:],
    )


def dot(a, b):
    return jnp.dot(a, b, preferred_element_type=jnp.float32)


def segments(pairs, outs, h_re, h_im, first, c2, s2, c3, s3, tc, ts, last):
    parity = lax.broadcasted_iota(jnp.int32, (1, N2), 1) % 2
    sign = (1 - 2 * parity).astype(jnp.float32)
    b_re = []
    b_im = []
    nyq = []
    for cur, prev in pairs:
        a = dot(first[...], jnp.concatenate([cur, prev], axis=0))
        a_re = a[:N1]
        a_im = a[N1:]
        b_re.append((a_re * tc[...] + a_im * ts[...]).astype(jnp.bfloat16))
        b_im.append((a_im * tc[...] - a_re * ts[...]).astype(jnp.bfloat16))
        nyq.append(jnp.sum(a_re[0:1] * sign, axis=1, keepdims=True))
    b_re = jnp.concatenate(b_re, axis=0)
    b_im = jnp.concatenate(b_im, axis=0)
    x_re = dot(b_re, c2[...]) + dot(b_im, s2[...])
    x_im = dot(b_im, c2[...]) - dot(b_re, s2[...])
    z_re = []
    z_im = []
    for i in range(len(pairs)):
        rows = slice(i * N1, (i + 1) * N1)
        hr = h_re[...]
        hi = h_im[...]
        z_re.append((x_re[rows] * hr - x_im[rows] * hi).astype(jnp.bfloat16))
        z_im.append((x_re[rows] * hi + x_im[rows] * hr).astype(jnp.bfloat16))
    z_re = jnp.concatenate(z_re, axis=0)
    z_im = jnp.concatenate(z_im, axis=0)
    p_re = dot(z_re, c3[...]) - dot(z_im, s3[...])
    p_im = dot(z_im, c3[...]) + dot(z_re, s3[...])
    for i, out in enumerate(outs):
        rows = slice(i * N1, (i + 1) * N1)
        q_re = (p_re[rows] * tc[...] - p_im[rows] * ts[...]).astype(jnp.bfloat16)
        q_im = (p_im[rows] * tc[...] + p_re[rows] * ts[...]).astype(jnp.bfloat16)
        total = dot(last[:, :N1], q_re) + dot(last[:, N1:], q_im)
        total = total + (nyq[i] * h_im[0:1, 0:1]) * sign
        out[...] = (total * (2.0 / FFT)).astype(jnp.bfloat16)


def filter_parts(recv, h_re, h_im):
    for p, ref in enumerate((h_re, h_im)):
        for rh in range(2):
            for kh in range(2):
                ref[rh * ROWS : (rh + 1) * ROWS, kh * LANES : (kh + 1) * LANES] = recv[
                    p * 4 + rh * 2 + kh, :, N2:
                ].astype(jnp.float32)


def inner_kernel(recv, by_column, by_row, twiddles, out, h_re, h_im):
    filter_parts(recv, h_re, h_im)
    consts = (h_re, h_im) + split_tables(by_column, by_row, twiddles)

    def step(i, carry):
        s = 2 * i + 1
        segments(
            [(recv[s, :, :N2], recv[s - 1, :, :N2]), (recv[s + 1, :, :N2], recv[s, :, :N2])],
            [out.at[s], out.at[s + 1]],
            *consts,
        )
        return carry

    lax.fori_loop(0, (SEGS - 2) // 2, step, 0, unroll=True)


def border_kernel(yh, acc, recv, border, h_re, h_im, by_column, by_row, twiddles, out):
    consts = (h_re, h_im) + split_tables(by_column, by_row, twiddles)
    before = jnp.where(yh[0] == 0, jnp.zeros_like(border), border[...])
    segments(
        [(recv[SEGS - 1, :, :N2], recv[SEGS - 2, :, :N2]), (recv[0, :, :N2], before)],
        [out.at[SEGS - 1], out.at[0]],
        *consts,
    )


MACS = 2 * N1 * N1 * N2 + 8 * N1 * N2 * HALF + ROWS * 2 * N1 * N2
IN_VMEM = pl.BlockSpec(memory_space=pltpu.VMEM)


def convolve(yh, recv, border, consts):
    params = pltpu.CompilerParams(vmem_limit_bytes=28 * 1024 * 1024)
    shape = jax.ShapeDtypeStruct((SEGS, ROWS, N2), jnp.bfloat16)
    part = jax.ShapeDtypeStruct((N1, HALF), jnp.float32)
    inner, h_re, h_im = pl.pallas_call(
        inner_kernel,
        in_specs=[IN_VMEM] * 4,
        out_specs=[IN_VMEM] * 3,
        out_shape=[shape, part, part],
        compiler_params=params,
        cost_estimate=pl.CostEstimate(flops=12 * MACS, bytes_accessed=4 << 20, transcendentals=0),
        name="inner",
    )(recv, *consts)
    return pl.pallas_call(
        border_kernel,
        in_specs=[pl.BlockSpec(memory_space=pltpu.SMEM)] + [IN_VMEM] * 8,
        out_specs=IN_VMEM,
        out_shape=shape,
        input_output_aliases={1: 0},
        compiler_params=params,
        cost_estimate=pl.CostEstimate(flops=4 * MACS, bytes_accessed=3 << 20, transcendentals=0),
        name="border",
    )(yh, inner, recv, border, h_re, h_im, *consts)


def hold_kernel(table, out):
    out[...] = table[...]


def hold(table):
    return pl.pallas_call(
        hold_kernel,
        in_specs=[IN_VMEM],
        out_specs=IN_VMEM,
        out_shape=jax.ShapeDtypeStruct(table.shape, table.dtype),
        compiler_params=pltpu.CompilerParams(vmem_limit_bytes=8 * 1024 * 1024),
        cost_estimate=pl.CostEstimate(flops=1 << 20, bytes_accessed=1 << 20, transcendentals=0),
        name="hold",
    )(table)


def edge_kernel(recv, out):
    out[...] = recv[SEGS - 1, :, :N2]


def edge(recv):
    return pl.pallas_call(
        edge_kernel,
        in_specs=[IN_VMEM],
        out_specs=IN_VMEM,
        out_shape=jax.ShapeDtypeStruct((ROWS, N2), jnp.bfloat16),
        compiler_params=pltpu.CompilerParams(vmem_limit_bytes=8 * 1024 * 1024),
        name="edge",
    )(recv)


CHUNKS = N2 // LANES
IN_SMEM = pl.BlockSpec(memory_space=pltpu.SMEM)
ANYWHERE = pl.BlockSpec(memory_space=pl.ANY)


def pack_kernel(sl, tok, value, gate_in, spectrum, out, vbuf, gbuf, pbuf, nbuf, turned, sems):
    part = sl[0] // 4
    rh = (sl[0] // 2) % 2
    kh = sl[0] % 2
    k_lanes = pl.ds(pl.multiple_of(kh * LANES, LANES), LANES)
    piece = pltpu.make_async_copy(
        spectrum.at[part, pl.ds(rh * ROW_T, ROW_T), k_lanes, :], pbuf, sems.at[2 * CHUNKS]
    )
    nyquist = pltpu.make_async_copy(
        spectrum.at[0, 0, pl.ds(HALF, 8), :], nbuf, sems.at[2 * CHUNKS + 1]
    )
    piece.start()
    nyquist.start()
    copies = []
    for j in range(CHUNKS):
        lanes = pl.ds(j * LANES, LANES)
        for i, (src, dst) in enumerate(((value, vbuf), (gate_in, gbuf))):
            copies.append(
                pltpu.make_async_copy(src.at[:, lanes, :], dst.at[:, lanes, :], sems.at[2 * j + i])
            )
            copies[-1].start()

    def place(j, row, v):
        turned[j % 2, pl.ds(row, LANES, stride=ROW_T), :] = v.T

    def write(j):
        lanes = slice(j * LANES, (j + 1) * LANES)
        out[:, :, lanes] = turned[j % 2].reshape(LANES, ROW_T, LANES).astype(jnp.bfloat16)

    piece.wait()
    nyquist.wait()
    mine = (tok[0] == 0) & (sl[0] % 4 == 0)
    for row in range(ROW_T):
        v = pbuf[row].astype(jnp.float32)
        if row == 0:
            edge = jnp.where(part == 0, v[0:1], nbuf[0:1].astype(jnp.float32))
            at_edge = (lax.broadcasted_iota(jnp.int32, v.shape, 0) == 0) & mine
            v = jnp.where(at_edge, 0.5 * edge, v)
        place(CHUNKS, row, v)
    write(CHUNKS)
    for j in range(CHUNKS):
        copies[2 * j].wait()
        copies[2 * j + 1].wait()
        lanes = slice(j * LANES, (j + 1) * LANES)
        for row in range(ROW_T):
            v = vbuf[row, lanes].astype(jnp.float32) * gbuf[row, lanes].astype(jnp.float32)
            place(j + 1, row, v.astype(jnp.bfloat16).astype(jnp.float32))
        out[:, :, lanes] = turned[(j + 1) % 2].reshape(LANES, ROW_T, LANES).astype(jnp.bfloat16)


def pack(sl, tok, value, gate_in, filter_spectrum):
    return pl.pallas_call(
        pack_kernel,
        in_specs=[IN_SMEM, IN_SMEM, ANYWHERE, ANYWHERE, ANYWHERE],
        out_specs=IN_VMEM,
        out_shape=jax.ShapeDtypeStruct((LANES, ROW_T, WIDE), jnp.bfloat16),
        scratch_shapes=[
            pltpu.VMEM((ROW_T, N2, LANES), jnp.bfloat16),
            pltpu.VMEM((ROW_T, N2, LANES), jnp.bfloat16),
            pltpu.VMEM((ROW_T, LANES, LANES), jnp.bfloat16),
            pltpu.VMEM((8, LANES), jnp.bfloat16),
            pltpu.VMEM((2, LANES * ROW_T, LANES), jnp.float32),
            pltpu.SemaphoreType.DMA((2 * CHUNKS + 2,)),
        ],
        cost_estimate=pl.CostEstimate(flops=1 << 20, bytes_accessed=3 << 20, transcendentals=0),
        name="pack",
    )(sl, tok, value, gate_in, filter_spectrum)


def finish_kernel(back, value, gate_in, gate_out, skip, out, turned, obuf, sems):
    copies = []
    for j in range(CHUNKS):
        lanes = slice(j * LANES, (j + 1) * LANES)
        slot = j % 2
        turned[slot] = back[:, :, lanes].astype(jnp.float32).reshape(LANES * ROW_T, LANES)
        for row in range(ROW_T):
            mixed = turned[slot, pl.ds(row, LANES, stride=ROW_T), :].T
            gated = value[row, lanes].astype(jnp.float32) * gate_in[row, lanes].astype(jnp.float32)
            gated = gated.astype(jnp.bfloat16).astype(jnp.float32)
            res = gate_out[row, lanes].astype(jnp.float32) * (mixed + skip[...] * gated)
            obuf[row, lanes] = res.astype(jnp.bfloat16)
        where = pl.ds(j * LANES, LANES)
        copies.append(
            pltpu.make_async_copy(obuf.at[:, where, :], out.at[:, where, :], sems.at[j])
        )
        copies[-1].start()
    for copy in copies:
        copy.wait()


def finish(back, value, gate_in, gate_out, skip):
    return pl.pallas_call(
        finish_kernel,
        in_specs=[IN_VMEM] * 5,
        out_specs=ANYWHERE,
        out_shape=jax.ShapeDtypeStruct((ROW_T, N2, LANES), jnp.bfloat16),
        scratch_shapes=[
            pltpu.VMEM((2, LANES * ROW_T, LANES), jnp.float32),
            pltpu.VMEM((ROW_T, N2, LANES), jnp.bfloat16),
            pltpu.SemaphoreType.DMA((CHUNKS,)),
        ],
        compiler_params=pltpu.CompilerParams(
            vmem_limit_bytes=14 * 1024 * 1024
        ),
        cost_estimate=pl.CostEstimate(flops=1 << 20, bytes_accessed=5 << 20, transcendentals=0),
        name="finish",
    )(back, value, gate_in, gate_out, skip)


def shards(value, gate_in, gate_out, filter_spectrum, skip_gain):
    sl = lax.axis_index(("x", "core")).reshape(1)
    tok = lax.axis_index(("z", "yl")).reshape(1)
    cut = lambda a: a.reshape(ROW_T, N2, LANES)
    value = cut(value)
    gate_in = cut(gate_in)
    gate_out = cut(gate_out)
    send = pack(sl, tok, value, gate_in, filter_spectrum)
    by_column, by_row, twiddles = tables()
    send, by_row = lax.optimization_barrier((send, by_row))
    recv = lax.all_to_all(send, GROUP, split_axis=0, concat_axis=0, tiled=True)
    recv = recv.reshape(SEGS, ROWS, WIDE)
    border = lax.ppermute(edge(recv), "yh", [(0, 1), (1, 0)])
    by_row = hold(by_row)
    mixed = convolve(lax.axis_index("yh").reshape(1), recv, border, (by_column, by_row, twiddles))
    back = lax.all_to_all(
        mixed.reshape(SEGS * 16, ROW_T, N2), GROUP, split_axis=0, concat_axis=0, tiled=True
    )
    result = finish(back, value, gate_in, gate_out, skip_gain.reshape(1, LANES))
    return result.reshape(-1, LANES)


def solution(mesh):
    fine = Mesh(mesh.devices.reshape(2, 4, 2, 8, 2), ALL)
    return jax.shard_map(
        shards,
        mesh=fine,
        in_specs=(
            P(ALL, None),
            P(ALL, None),
            P(ALL, None),
            P(None, ("z", "yl"), None, None),
            P(),
        ),
        out_specs=P(ALL, None),
        check_vma=False,
    )
```
